32 devices in a mesh: rep: 2 (over z, core), dp: 16 (over x, y).
Axes of the slice: x: 4, y: 4, z: 1, core: 2. Of those that a mesh axis runs over, the one named last changes fastest.
The devices are a block of a 4x4x8 slice.
Arguments:
- g_w_gate: bfloat16 [32, 2, 896, 2560], P(('rep', 'dp')), parts along dimension 0
- g_w_up: bfloat16 [32, 2, 896, 2560], P(('rep', 'dp')), parts along dimension 0
- g_w_down: bfloat16 [32, 2, 2560, 896], P(('rep', 'dp')), parts along dimension 0
- w_gate: bfloat16 [2, 896, 2560], replicated
- w_up: bfloat16 [2, 896, 2560], replicated
- w_down: bfloat16 [2, 2560, 896], replicated
- m_w_gate: float32 [2, 896, 2560], P(None, 'dp')
- m_w_up: float32 [2, 896, 2560], P(None, 'dp')
- m_w_down: float32 [2, 2560, 896], P(None, 'dp')
- v_w_gate: float32 [2, 896, 2560], P(None, 'dp')
- v_w_up: float32 [2, 896, 2560], P(None, 'dp')
- v_w_down: float32 [2, 2560, 896], P(None, 'dp')
Outputs:
- output 1: bfloat16 [4, 896, 2560], P('rep'), parts along dimension 0
- output 2: bfloat16 [4, 896, 2560], P('rep'), parts along dimension 0
- output 3: bfloat16 [4, 2560, 896], P('rep'), parts along dimension 0
- output 4: float32 [4, 896, 2560], P('rep', 'dp'), parts along dimension 0
- output 5: float32 [4, 896, 2560], P('rep', 'dp'), parts along dimension 0
- output 6: float32 [4, 2560, 896], P('rep', 'dp'), parts along dimension 0
- output 7: float32 [4, 896, 2560], P('rep', 'dp'), parts along dimension 0
- output 8: float32 [4, 896, 2560], P('rep', 'dp'), parts along dimension 0
- output 9: float32 [4, 2560, 896], P('rep', 'dp'), parts along dimension 0
There are 2 independent parts. The reference program is written for one: setup_inputs(seed, part) draws one part's arguments, and reference() takes and returns one part's arrays. A program takes and returns all parts, laid end to end along the dimension named above; an argument that names none is the same for every part.
All inputs are finite; a program needn't handle non-finite values.
Results may differ from the reference program's by a relative error of at most 0.022.
Values are sent between devices in bfloat16 or wider.
A program may use at most 768 MiB of HBM per device.

```python
import jax
import jax.numpy as jnp
from jax import lax

DEVICES = 16
D = 896
FF = 2560
LAYERS = 2
NAMES = ("w_gate", "w_up", "w_down")
SHAPES = {"w_gate": (LAYERS, D, FF), "w_up": (LAYERS, D, FF), "w_down": (LAYERS, FF, D)}


def setup_inputs(seed: int = 0, part: int = 0) -> dict:
    kz, *keys = jax.random.split(jax.random.key(seed), 1 + 5 * len(NAMES))
    loud = 2.0 ** jax.random.uniform(kz, (), jnp.float32, -1.0, 1.0)
    drawn = {}
    for name, key, both in zip(NAMES, keys[:3], keys[3:6], strict=True):
        own = jax.random.normal(jax.random.fold_in(key, part), (DEVICES, *SHAPES[name]), jnp.float32)
        shared = jax.random.normal(jax.random.fold_in(both, part), SHAPES[name], jnp.float32)
        drawn["g_" + name] = (loud * (0.7 * shared / DEVICES + 0.7 * own * DEVICES**-0.5)).astype(jnp.bfloat16)
    for name, key in zip(NAMES, keys[6:9], strict=True):
        drawn[name] = (jax.random.normal(key, SHAPES[name], jnp.float32) * SHAPES[name][1] ** -0.5).astype(jnp.bfloat16)
    for name, key in zip(NAMES, keys[9:12], strict=True):
        drawn["m_" + name] = loud * 0.5 * jax.random.normal(key, SHAPES[name], jnp.float32)
    for name, key in zip(NAMES, keys[12:15], strict=True):
        drawn["v_" + name] = loud * loud * jax.random.uniform(key, SHAPES[name], jnp.float32, 0.5, 1.5)
    return drawn


def adamw(w, m, v, g):
    m = 0.9 * m + 0.1 * g
    v = 0.95 * v + 0.05 * g * g
    step = m * lax.rsqrt(v + 1e-8) + 0.1 * w
    return (w - 0.02 * step).astype(jnp.bfloat16), m, v


def clipped(gradients, sum_of_squares, count):
    factor = jnp.minimum(1.0, 0.5 * lax.rsqrt(sum_of_squares / count + 1e-30))
    return [g * factor for g in gradients]


def reference(g_w_gate, g_w_up, g_w_down, w_gate, w_up, w_down, m_w_gate, m_w_up, m_w_down, v_w_gate, v_w_up, v_w_down):
    def total(terms):
        return lax.scan(lambda so_far, term: (so_far + term.astype(jnp.float32), None), jnp.zeros(terms.shape[1:], jnp.float32), terms)[0]

    gradients = [total(terms).astype(jnp.bfloat16).astype(jnp.float32) for terms in (g_w_gate, g_w_up, g_w_down)]
    gradients = clipped(gradients, sum(jnp.sum(g * g) for g in gradients), sum(g.size for g in gradients))
    new = [
        adamw(w.astype(jnp.float32), m, v, g)
        for w, m, v, g in zip((w_gate, w_up, w_down), (m_w_gate, m_w_up, m_w_down), (v_w_gate, v_w_up, v_w_down), gradients, strict=True)
    ]
    return tuple(one[which] for which in range(3) for one in new)
```

```python
import functools
import math

import jax
import jax.numpy as jnp
from jax import lax
from jax.experimental import pallas as pl
from jax.experimental.pallas import tpu as pltpu
from jax.sharding import PartitionSpec as P

MESH = pl.DeviceIdType.MESH
COLOURS = 4


def tiled(a, lead):
    rows, columns = a.shape[-2:]
    t = a.reshape(*a.shape[:-2], rows // 8, 8, columns // 128, 128)
    return jnp.swapaxes(t, -3, -2).reshape(*lead, -1, 8, 128)


def untiled(t, shape):
    rows, columns = shape[-2:]
    t = t.reshape(*shape[:-2], rows // 8, columns // 128, 8, 128)
    return jnp.swapaxes(t, -3, -2).reshape(shape)


def step_kernel(side, layers, count, *refs):
    n = side * side
    terms, weights, m_in, v_in = (refs[i : i + 3] for i in (0, 3, 6, 9))
    whole, m_ref, v_ref, first, second, own_w, squares, total, load, load3, send, recv, sq_send, sq_recv = refs[12:]
    pieces = whole.shape[0]
    tiles = whole.shape[3]
    part = tiles // COLOURS
    hops = side - 1
    me = lax.axis_index("dp")
    x, y = me // side, me % side

    def load_terms(piece):
        return pltpu.make_async_copy(terms[piece // layers].at[piece % layers], whole.at[piece], load.at[piece])

    def load_state(piece):
        a, l = piece // layers, piece % layers
        return (
            pltpu.make_async_copy(weights[a].at[l, x, y], own_w.at[piece], load3.at[0, piece]),
            pltpu.make_async_copy(m_in[a].at[l], m_ref.at[piece], load3.at[1, piece]),
            pltpu.make_async_copy(v_in[a].at[l], v_ref.at[piece], load3.at[2, piece]),
        )

    for piece in range(pieces):
        load_terms(piece).start()

    barrier = pltpu.get_barrier_semaphore()

    @pl.loop(1, n)
    def _(i):
        pl.semaphore_signal(barrier, inc=1, device_id={"dp": (me + i) % n}, device_id_type=MESH)

    pl.semaphore_wait(barrier, n - 1)

    def place(c):
        way = 1 if c % 2 == 0 else -1
        return (x, y, way) if c < 2 else (y, x, way)

    def device(c, p, q):
        return p * side + q if c < 2 else q * side + p

    def row(c, piece, p):
        cut = pl.ds(c * part, part)
        return whole.at[piece, p, :, cut] if c < 2 else whole.at[piece, :, p, cut]

    def block(c, piece, p, q):
        cut = pl.ds(c * part, part)
        return whole.at[piece, p, q, cut] if c < 2 else whole.at[piece, q, p, cut]

    def wrap(i):
        return (i + 2 * side) % side

    def scatter(c, k, piece):
        p, q, way = place(c)
        if k < hops:
            source, target = row(c, piece, wrap(p - way * (k + 1))), first.at[k, c, piece]
            to = device(c, wrap(p + way), q)
        else:
            source, target = block(c, piece, p, wrap(q - way * (k - hops + 1))), second.at[k - hops, c, piece]
            to = device(c, p, wrap(q + way))
        return pltpu.make_async_remote_copy(
            src_ref=source, dst_ref=target, send_sem=send.at[k, c, piece], recv_sem=recv.at[k, c, piece], device_id={"dp": to}, device_id_type=MESH
        )

    def add(c, k, piece):
        p, q, way = place(c)
        if k < hops:
            mine, came = row(c, piece, wrap(p - way * (k + 2))), first.at[k, c, piece]

            @pl.loop(0, side)
            def _(i):
                mine[i] = (mine[i].astype(jnp.float32) + came[i].astype(jnp.float32)).astype(jnp.bfloat16)

        else:
            mine, came = block(c, piece, p, wrap(q - way * (k - hops + 2))), second.at[k - hops, c, piece]
            new = (mine[...].astype(jnp.float32) + came[...].astype(jnp.float32)).astype(jnp.bfloat16)
            mine[...] = new
            if k == 2 * hops - 1:
                g = new.astype(jnp.float32)
                total[...] += jnp.sum(g * g, axis=0)

    total[...] = jnp.zeros_like(total)

    for piece in range(pieces):
        load_terms(piece).wait()
        for c in range(COLOURS):
            scatter(c, 0, piece).start()
    for piece in range(pieces):
        for copy in load_state(piece):
            copy.start()

    last = COLOURS - 1
    for k in range(2 * hops):

        @pl.loop(0, pieces)
        def _(piece, k=k):
            for c in range(COLOURS):
                scatter(c, k, piece).wait_recv()
                add(c, k, piece)
                if c:
                    if k + 1 < 2 * hops:
                        scatter(c - 1, k + 1, piece).start()
                    continue

                if k + 1 < 2 * hops:

                    @pl.when(piece > 0)
                    def _():
                        scatter(last, k + 1, piece - 1).start()

                if k:

                    @pl.when(piece == 0)
                    def _():
                        scatter(last, k, pieces - 1).start()

    for k in range(2 * hops):

        @pl.loop(0, pieces)
        def _(piece, k=k):
            for c in range(COLOURS):
                scatter(c, k, piece).wait_send()

    def tell(i):
        return pltpu.make_async_remote_copy(
            src_ref=total, dst_ref=squares.at[i], send_sem=sq_send.at[i], recv_sem=sq_recv.at[i], device_id={"dp": (me + i) % n}, device_id_type=MESH
        )

    @pl.loop(1, n)
    def _(i):
        tell(i).start()

    squares[0] = total[...]
    for piece in range(pieces):
        for copy in load_state(piece):
            copy.wait()

    @pl.loop(1, n)
    def _(i):
        tell(i).wait_recv()

    of_all = jnp.sum(jnp.sum(squares[...], axis=0), keepdims=True)
    factor = jnp.minimum(1.0, 0.5 * lax.rsqrt(of_all / count + 1e-30))[None]

    def gather(c, k, piece):
        p, q, way = place(c)
        if k < hops:
            moved, to = block(c, piece, p, wrap(q - way * k)), device(c, p, wrap(q + way))
        else:
            moved, to = row(c, piece, wrap(p - way * (k - hops))), device(c, wrap(p + way), q)
        return pltpu.make_async_remote_copy(
            src_ref=moved, dst_ref=moved, send_sem=send.at[k, c, piece], recv_sem=recv.at[k, c, piece], device_id={"dp": to}, device_id_type=MESH
        )

    @pl.loop(0, pieces)
    def _(piece):
        mine = whole.at[piece, x, y]

        @pl.loop(0, COLOURS)
        def _(c):
            cut = pl.ds(c * part, part)
            g = mine[cut].astype(jnp.float32) * factor
            w = own_w[piece, cut].astype(jnp.float32)
            m = 0.9 * m_ref[piece, cut] + 0.1 * g
            v = 0.95 * v_ref[piece, cut] + 0.05 * g * g
            m_ref[piece, cut] = m
            v_ref[piece, cut] = v
            mine[cut] = (w - 0.02 * (m * lax.rsqrt(v + 1e-8) + 0.1 * w)).astype(jnp.bfloat16)

        @pl.when(piece > 0)
        def _():
            for c in range(COLOURS):
                gather(c, 0, piece - 1).start()

    for k in range(2 * hops):

        @pl.loop(0, pieces)
        def _(piece, k=k):
            for c in range(COLOURS):
                gather(c, k, piece).wait_recv()
                if k + 1 < 2 * hops:
                    gather(c, k + 1, piece).start()
            if k == 0:

                @pl.when(piece == 0)
                def _():
                    for c in range(COLOURS):
                        gather(c, 0, pieces - 1).start()

    for k in range(2 * hops):

        @pl.loop(0, pieces)
        def _(piece, k=k):
            for c in range(COLOURS):
                gather(c, k, piece).wait_send()

    @pl.loop(1, n)
    def _(i):
        tell(i).wait_send()


def out_kernel(layers, whole, m_ref, v_ref, *refs):
    outs, sems = refs[:9], refs[9]
    copies = [
        pltpu.make_async_copy(source.at[3 * 0 + piece], outs[3 * i + piece // layers].at[piece % layers], sems.at[i, piece])
        for i, source in enumerate((whole, m_ref, v_ref))
        for piece in range(3 * layers)
    ]
    for copy in copies:
        copy.start()
    for copy in copies:
        copy.wait()


def solution(mesh):
    n = mesh.shape["dp"]
    side = math.isqrt(n)

    def step(*arrays):
        terms, weights, m, v = (arrays[i : i + 3] for i in (0, 3, 6, 9))
        layers = weights[0].shape[0]
        pieces = 3 * layers
        terms = [tiled(t[0], (layers, side, side)) for t in terms]
        whole = [tiled(w, (layers, side, side)) for w in weights]
        ms = [tiled(one, (layers,)) for one in m]
        vs = [tiled(one, (layers,)) for one in v]
        tiles = ms[0].shape[1]
        part = tiles // COLOURS
        assert side * side == n and tiles % COLOURS == 0 and all(one.shape[1] == tiles for one in ms)
        hops = side - 1
        any_space = pl.BlockSpec(memory_space=pl.ANY)
        vmem = pl.BlockSpec(memory_space=pltpu.VMEM)
        bf16, f32, dma = jnp.bfloat16, jnp.float32, pltpu.SemaphoreType.DMA
        count = float(sum(w.size for w in weights))
        new = pl.pallas_call(
            functools.partial(step_kernel, side, layers, count),
            out_shape=(
                pltpu.VMEM((pieces, side, side, tiles, 8, 128), bf16),
                pltpu.VMEM((pieces, tiles, 8, 128), f32),
                pltpu.VMEM((pieces, tiles, 8, 128), f32),
            ),
            in_specs=[any_space] * 12,
            out_specs=(vmem,) * 3,
            scratch_shapes=[
                pltpu.VMEM((hops, COLOURS, pieces, side, part, 8, 128), bf16),
                pltpu.VMEM((hops, COLOURS, pieces, part, 8, 128), bf16),
                pltpu.VMEM((pieces, tiles, 8, 128), bf16),
                pltpu.VMEM((n, 8, 128), f32),
                pltpu.VMEM((8, 128), f32),
                dma((pieces,)),
                dma((3, pieces)),
                dma((2 * hops, COLOURS, pieces)),
                dma((2 * hops, COLOURS, pieces)),
                dma((n,)),
                dma((n,)),
            ],
            compiler_params=pltpu.CompilerParams(collective_id=0, has_side_effects=True, vmem_limit_bytes=27 * 2**20),
            name="step",
        )(*terms, *whole, *ms, *vs)
        return finish(new, layers, weights, m, v)
        shapes = [(layers, side, side, tiles, 8, 128)] * 3 + [(layers, tiles, 8, 128)] * 6
        outs = pl.pallas_call(
            functools.partial(out_kernel, layers),
            out_shape=[jax.ShapeDtypeStruct(s, bf16 if i < 3 else f32) for i, s in enumerate(shapes)],
            in_specs=[vmem] * 3,
            out_specs=[any_space] * 9,
            scratch_shapes=[dma((3, pieces))],
            compiler_params=pltpu.CompilerParams(vmem_limit_bytes=2**20),
            name="out",
        )(*new)
        return tuple(untiled(one, like.shape) for one, like in zip(outs, (*weights, *m, *v), strict=True))

    all_of, cut = P(None, None, None), P(None, "dp", None)
    return jax.shard_map(
        step,
        mesh=mesh,
        in_specs=(P(("rep", "dp"), None, None, None),) * 3 + (all_of,) * 3 + (cut,) * 6,
        out_specs=(P("rep", None, None),) * 3 + (P("rep", "dp", None),) * 6,
        check_vma=False,
    )

def finish(new, layers, weights, m, v):
    outs = [one[layers * a : layers * (a + 1)] for one in new for a in range(3)]
    return tuple(untiled(one, like.shape) for one, like in zip(outs, (*weights, *m, *v), strict=True))
```

```python
import functools
import math

import jax
import jax.numpy as jnp
from jax import lax
from jax.experimental import pallas as pl
from jax.experimental.pallas import tpu as pltpu
from jax.sharding import PartitionSpec as P

MESH = pl.DeviceIdType.MESH
COLOURS = 4


def tiled(a, lead):
    rows, columns = a.shape[-2:]
    t = a.reshape(*a.shape[:-2], rows // 8, 8, columns // 128, 128)
    return jnp.swapaxes(t, -3, -2).reshape(*lead, -1, 8, 128)


def untiled(t, shape):
    rows, columns = shape[-2:]
    t = t.reshape(*shape[:-2], rows // 8, columns // 128, 8, 128)
    return jnp.swapaxes(t, -3, -2).reshape(shape)


def step_kernel(side, layers, count, *refs):
    n = side * side
    terms, weights, m_in, v_in = (refs[i : i + 3] for i in (0, 3, 6, 9))
    state, whole, first, second, own_w, squares, total, load, load3, send, recv, sq_send, sq_recv = refs[12:]
    m_ref, v_ref = state.at[0], state.at[1]
    pieces = whole.shape[0]
    tiles = whole.shape[3]
    part = tiles // COLOURS
    hops = side - 1
    me = lax.axis_index("dp")
    x, y = me // side, me % side

    def load_terms(piece):
        return pltpu.make_async_copy(terms[piece // layers].at[piece % layers], whole.at[piece], load.at[piece])

    def load_state(piece):
        a, l = piece // layers, piece % layers
        return (
            pltpu.make_async_copy(weights[a].at[l, x, y], own_w.at[piece], load3.at[0, piece]),
            pltpu.make_async_copy(m_in[a].at[l], m_ref.at[piece], load3.at[1, piece]),
            pltpu.make_async_copy(v_in[a].at[l], v_ref.at[piece], load3.at[2, piece]),
        )

    for piece in range(pieces):
        load_terms(piece).start()

    barrier = pltpu.get_barrier_semaphore()

    @pl.loop(1, n)
    def _(i):
        pl.semaphore_signal(barrier, inc=1, device_id={"dp": (me + i) % n}, device_id_type=MESH)

    pl.semaphore_wait(barrier, n - 1)

    def place(c):
        way = 1 if c % 2 == 0 else -1
        return (x, y, way) if c < 2 else (y, x, way)

    def device(c, p, q):
        return p * side + q if c < 2 else q * side + p

    def row(c, piece, p):
        cut = pl.ds(c * part, part)
        return whole.at[piece, p, :, cut] if c < 2 else whole.at[piece, :, p, cut]

    def block(c, piece, p, q):
        cut = pl.ds(c * part, part)
        return whole.at[piece, p, q, cut] if c < 2 else whole.at[piece, q, p, cut]

    def wrap(i):
        return (i + 2 * side) % side

    def scatter(c, k, piece):
        p, q, way = place(c)
        if k < hops:
            source, target = row(c, piece, wrap(p - way * (k + 1))), first.at[k, c, piece]
            to = device(c, wrap(p + way), q)
        else:
            source, target = block(c, piece, p, wrap(q - way * (k - hops + 1))), second.at[k - hops, c, piece]
            to = device(c, p, wrap(q + way))
        return pltpu.make_async_remote_copy(
            src_ref=source, dst_ref=target, send_sem=send.at[k, c, piece], recv_sem=recv.at[k, c, piece], device_id={"dp": to}, device_id_type=MESH
        )

    def add(c, k, piece):
        p, q, way = place(c)
        if k < hops:
            mine, came = row(c, piece, wrap(p - way * (k + 2))), first.at[k, c, piece]

            @pl.loop(0, side)
            def _(i):
                mine[i] = (mine[i].astype(jnp.float32) + came[i].astype(jnp.float32)).astype(jnp.bfloat16)

        else:
            mine, came = block(c, piece, p, wrap(q - way * (k - hops + 2))), second.at[k - hops, c, piece]
            new = (mine[...].astype(jnp.float32) + came[...].astype(jnp.float32)).astype(jnp.bfloat16)
            mine[...] = new
            if k == 2 * hops - 1:
                g = new.astype(jnp.float32)
                total[...] += jnp.sum(g * g, axis=0)

    total[...] = jnp.zeros_like(total)

    for piece in range(pieces):
        load_terms(piece).wait()
        for c in range(COLOURS):
            scatter(c, 0, piece).start()
    for piece in range(pieces):
        for copy in load_state(piece):
            copy.start()

    last = COLOURS - 1
    for k in range(2 * hops):

        @pl.loop(0, pieces)
        def _(piece, k=k):
            for c in range(COLOURS):
                scatter(c, k, piece).wait_recv()
                add(c, k, piece)
                if c:
                    if k + 1 < 2 * hops:
                        scatter(c - 1, k + 1, piece).start()
                    continue

                if k + 1 < 2 * hops:

                    @pl.when(piece > 0)
                    def _():
                        scatter(last, k + 1, piece - 1).start()

                if k:

                    @pl.when(piece == 0)
                    def _():
                        scatter(last, k, pieces - 1).start()

    for k in range(2 * hops):

        @pl.loop(0, pieces)
        def _(piece, k=k):
            for c in range(COLOURS):
                scatter(c, k, piece).wait_send()

    def tell(i):
        return pltpu.make_async_remote_copy(
            src_ref=total, dst_ref=squares.at[i], send_sem=sq_send.at[i], recv_sem=sq_recv.at[i], device_id={"dp": (me + i) % n}, device_id_type=MESH
        )

    @pl.loop(1, n)
    def _(i):
        tell(i).start()

    squares[0] = total[...]
    for piece in range(pieces):
        for copy in load_state(piece):
            copy.wait()

    @pl.loop(1, n)
    def _(i):
        tell(i).wait_recv()

    of_all = jnp.sum(jnp.sum(squares[...], axis=0), keepdims=True)
    factor = jnp.minimum(1.0, 0.5 * lax.rsqrt(of_all / count + 1e-30))[None]

    def gather(c, k, piece):
        p, q, way = place(c)
        if k < hops:
            moved, to = block(c, piece, p, wrap(q - way * k)), device(c, p, wrap(q + way))
        else:
            moved, to = row(c, piece, wrap(p - way * (k - hops))), device(c, wrap(p + way), q)
        return pltpu.make_async_remote_copy(
            src_ref=moved, dst_ref=moved, send_sem=send.at[k, c, piece], recv_sem=recv.at[k, c, piece], device_id={"dp": to}, device_id_type=MESH
        )

    @pl.loop(0, pieces)
    def _(piece):
        mine = whole.at[piece, x, y]

        @pl.loop(0, COLOURS)
        def _(c):
            cut = pl.ds(c * part, part)
            g = mine[cut].astype(jnp.float32) * factor
            w = own_w[piece, cut].astype(jnp.float32)
            m = 0.9 * m_ref[piece, cut] + 0.1 * g
            v = 0.95 * v_ref[piece, cut] + 0.05 * g * g
            m_ref[piece, cut] = m
            v_ref[piece, cut] = v
            mine[cut] = (w - 0.02 * (m * lax.rsqrt(v + 1e-8) + 0.1 * w)).astype(jnp.bfloat16)

        @pl.when(piece > 0)
        def _():
            for c in range(COLOURS):
                gather(c, 0, piece - 1).start()

    for k in range(2 * hops):

        @pl.loop(0, pieces)
        def _(piece, k=k):
            for c in range(COLOURS):
                gather(c, k, piece).wait_recv()
                if k + 1 < 2 * hops:
                    gather(c, k + 1, piece).start()
            if k == 0:

                @pl.when(piece == 0)
                def _():
                    for c in range(COLOURS):
                        gather(c, 0, pieces - 1).start()

    for k in range(2 * hops):

        @pl.loop(0, pieces)
        def _(piece, k=k):
            for c in range(COLOURS):
                gather(c, k, piece).wait_send()

    @pl.loop(1, n)
    def _(i):
        tell(i).wait_send()


def out_kernel(layers, state, whole, *refs):
    outs, sems = refs[:9], refs[9]
    copies = [
        pltpu.make_async_copy(source.at[piece], outs[3 * i + piece // layers].at[piece % layers], sems.at[i, piece])
        for i, source in enumerate((whole, state.at[0], state.at[1]))
        for piece in range(3 * layers)
    ]
    for copy in copies:
        copy.start()
    for copy in copies:
        copy.wait()


def solution(mesh):
    n = mesh.shape["dp"]
    side = math.isqrt(n)

    def step(*arrays):
        terms, weights, m, v = (arrays[i : i + 3] for i in (0, 3, 6, 9))
        layers = weights[0].shape[0]
        pieces = 3 * layers
        terms = [tiled(t[0], (layers, side, side)) for t in terms]
        whole = [tiled(w, (layers, side, side)) for w in weights]
        ms = [tiled(one, (layers,)) for one in m]
        vs = [tiled(one, (layers,)) for one in v]
        tiles = ms[0].shape[1]
        part = tiles // COLOURS
        assert side * side == n and tiles % COLOURS == 0 and all(one.shape[1] == tiles for one in ms)
        hops = side - 1
        any_space = pl.BlockSpec(memory_space=pl.ANY)
        vmem = pl.BlockSpec(memory_space=pltpu.VMEM)
        bf16, f32, dma = jnp.bfloat16, jnp.float32, pltpu.SemaphoreType.DMA
        count = float(sum(w.size for w in weights))
        new = pl.pallas_call(
            functools.partial(step_kernel, side, layers, count),
            out_shape=(
                pltpu.VMEM((2, pieces, tiles, 8, 128), f32),
                pltpu.VMEM((pieces, side, side, tiles, 8, 128), bf16),
            ),
            in_specs=[any_space] * 12,
            out_specs=(vmem,) * 2,
            scratch_shapes=[
                pltpu.VMEM((hops, COLOURS, pieces, side, part, 8, 128), bf16),
                pltpu.VMEM((hops, COLOURS, pieces, part, 8, 128), bf16),
                pltpu.VMEM((pieces, tiles, 8, 128), bf16),
                pltpu.VMEM((n, 8, 128), f32),
                pltpu.VMEM((8, 128), f32),
                dma((pieces,)),
                dma((3, pieces)),
                dma((2 * hops, COLOURS, pieces)),
                dma((2 * hops, COLOURS, pieces)),
                dma((n,)),
                dma((n,)),
            ],
            compiler_params=pltpu.CompilerParams(collective_id=0, has_side_effects=True, vmem_limit_bytes=27 * 2**20),
            name="step",
        )(*terms, *whole, *ms, *vs)
        new = [pltpu.with_memory_space_constraint(one, pltpu.VMEM) for one in new]
        shapes = [(layers, side, side, tiles, 8, 128)] * 3 + [(layers, tiles, 8, 128)] * 6
        outs = pl.pallas_call(
            functools.partial(out_kernel, layers),
            out_shape=[jax.ShapeDtypeStruct(s, bf16 if i < 3 else f32) for i, s in enumerate(shapes)],
            in_specs=[vmem] * 2,
            out_specs=[any_space] * 9,
            scratch_shapes=[dma((3, pieces))],
            compiler_params=pltpu.CompilerParams(vmem_limit_bytes=2**20),
            name="out",
        )(*new)
        return tuple(untiled(one, like.shape) for one, like in zip(outs, (*weights, *m, *v), strict=True))

    all_of, cut = P(None, None, None), P(None, "dp", None)
    return jax.shard_map(
        step,
        mesh=mesh,
        in_specs=(P(("rep", "dp"), None, None, None),) * 3 + (all_of,) * 3 + (cut,) * 6,
        out_specs=(P("rep", None, None),) * 3 + (P("rep", "dp", None),) * 6,
        check_vma=False,
    )
```

```python
import functools
import math

import jax
import jax.numpy as jnp
from jax import lax
from jax.experimental import pallas as pl
from jax.experimental.pallas import tpu as pltpu
from jax.sharding import PartitionSpec as P

MESH = pl.DeviceIdType.MESH
COLOURS = 4


def tiled(a, lead):
    rows, columns = a.shape[-2:]
    t = a.reshape(*a.shape[:-2], rows // 8, 8, columns // 128, 128)
    return jnp.swapaxes(t, -3, -2).reshape(*lead, -1, 8, 128)


def untiled(t, shape):
    rows, columns = shape[-2:]
    t = t.reshape(*shape[:-2], rows // 8, columns // 128, 8, 128)
    return jnp.swapaxes(t, -3, -2).reshape(shape)


def step_kernel(side, layers, count, *refs):
    n = side * side
    terms, weights, m_in, v_in = (refs[i : i + 3] for i in (0, 3, 6, 9))
    state, whole, first, second, own_w, squares, total, load, load3, send, recv, sq_send, sq_recv = refs[12:]
    m_ref, v_ref = state.at[0], state.at[1]
    pieces = whole.shape[0]
    tiles = whole.shape[3]
    part = tiles // COLOURS
    hops = side - 1
    me = lax.axis_index("dp")
    x, y = me // side, me % side

    def load_terms(piece):
        return pltpu.make_async_copy(terms[piece // layers].at[piece % layers], whole.at[piece], load.at[piece])

    def load_state(piece):
        a, l = piece // layers, piece % layers
        return (
            pltpu.make_async_copy(weights[a].at[l, x, y], own_w.at[piece], load3.at[0, piece]),
            pltpu.make_async_copy(m_in[a].at[l], m_ref.at[piece], load3.at[1, piece]),
            pltpu.make_async_copy(v_in[a].at[l], v_ref.at[piece], load3.at[2, piece]),
        )

    for piece in range(pieces):
        load_terms(piece).start()

    barrier = pltpu.get_barrier_semaphore()

    def place(c):
        way = 1 if c % 2 == 0 else -1
        return (x, y, way) if c < 2 else (y, x, way)

    def device(c, p, q):
        return p * side + q if c < 2 else q * side + p

    for c in range(COLOURS):
        p, q, way = place(c)
        pl.semaphore_signal(barrier, inc=1, device_id={"dp": device(c, (p + way + side) % side, q)}, device_id_type=MESH)
    pl.semaphore_wait(barrier, COLOURS)

    def row(c, piece, p):
        cut = pl.ds(c * part, part)
        return whole.at[piece, p, :, cut] if c < 2 else whole.at[piece, :, p, cut]

    def block(c, piece, p, q):
        cut = pl.ds(c * part, part)
        return whole.at[piece, p, q, cut] if c < 2 else whole.at[piece, q, p, cut]

    def wrap(i):
        return (i + 2 * side) % side

    def scatter(c, k, piece, own=None):
        p, q, way = place(c)
        if k < hops:
            source, target = row(c, piece, wrap(p - way * (k + 1))), first.at[k, c, piece]
            to = device(c, wrap(p + way), q)
            if own is not None:
                cut = pl.ds(c * part, part)
                own, i = own.at[piece % layers], wrap(p - way)
                source = own.at[i, :, cut] if c < 2 else own.at[:, i, cut]
        else:
            source, target = block(c, piece, p, wrap(q - way * (k - hops + 1))), second.at[k - hops, c, piece]
            to = device(c, p, wrap(q + way))
        return pltpu.make_async_remote_copy(
            src_ref=source, dst_ref=target, send_sem=send.at[k, c, piece], recv_sem=recv.at[k, c, piece], device_id={"dp": to}, device_id_type=MESH
        )

    def add(c, k, piece):
        p, q, way = place(c)
        if k < hops:
            mine, came = row(c, piece, wrap(p - way * (k + 2))), first.at[k, c, piece]

            @pl.loop(0, side)
            def _(i):
                mine[i] = (mine[i].astype(jnp.float32) + came[i].astype(jnp.float32)).astype(jnp.bfloat16)

        else:
            mine, came = block(c, piece, p, wrap(q - way * (k - hops + 2))), second.at[k - hops, c, piece]
            new = (mine[...].astype(jnp.float32) + came[...].astype(jnp.float32)).astype(jnp.bfloat16)
            mine[...] = new
            if k == 2 * hops - 1:
                g = new.astype(jnp.float32)
                total[...] += jnp.sum(g * g, axis=0)

    total[...] = jnp.zeros_like(total)

    for piece in range(pieces):
        for c in range(COLOURS):
            scatter(c, 0, piece, terms[piece // layers]).start()
    for piece in range(pieces):
        for copy in load_state(piece):
            copy.start()

    last = COLOURS - 1
    for k in range(2 * hops):

        @pl.loop(0, pieces)
        def _(piece, k=k):
            if k == 0:
                pltpu.make_async_copy(whole.at[piece], whole.at[piece], load.at[piece]).wait()
            for c in range(COLOURS):
                scatter(c, k, piece).wait_recv()
                add(c, k, piece)
                if k:
                    scatter(c, k - 1, piece).wait_send()
                if c:
                    if k + 1 < 2 * hops:
                        scatter(c - 1, k + 1, piece).start()
                    continue

                if k + 1 < 2 * hops:

                    @pl.when(piece > 0)
                    def _():
                        scatter(last, k + 1, piece - 1).start()

                if k:

                    @pl.when(piece == 0)
                    def _():
                        scatter(last, k, pieces - 1).start()

    def tell(i):
        return pltpu.make_async_remote_copy(
            src_ref=total, dst_ref=squares.at[i], send_sem=sq_send.at[i], recv_sem=sq_recv.at[i], device_id={"dp": (me + i) % n}, device_id_type=MESH
        )

    @pl.loop(1, n)
    def _(i):
        tell(i).start()

    squares[0] = total[...]

    @pl.loop(0, pieces)
    def _(piece):
        for c in range(COLOURS):
            scatter(c, 2 * hops - 1, piece).wait_send()

    for piece in range(pieces):
        for copy in load_state(piece):
            copy.wait()

    @pl.loop(1, n)
    def _(i):
        tell(i).wait_recv()

    of_all = jnp.sum(jnp.sum(squares[...], axis=0), keepdims=True)
    factor = jnp.minimum(1.0, 0.5 * lax.rsqrt(of_all / count + 1e-30))[None]

    def gather(c, k, piece):
        p, q, way = place(c)
        if k < hops:
            moved, to = block(c, piece, p, wrap(q - way * k)), device(c, p, wrap(q + way))
        else:
            moved, to = row(c, piece, wrap(p - way * (k - hops))), device(c, wrap(p + way), q)
        return pltpu.make_async_remote_copy(
            src_ref=moved, dst_ref=moved, send_sem=send.at[k, c, piece], recv_sem=recv.at[k, c, piece], device_id={"dp": to}, device_id_type=MESH
        )

    @pl.loop(0, pieces)
    def _(piece):
        mine = whole.at[piece, x, y]
        for c in range(COLOURS):
            cut = pl.ds(c * part, part)
            g = mine[cut].astype(jnp.float32) * factor
            w = own_w[piece, cut].astype(jnp.float32)
            m = 0.9 * m_ref[piece, cut] + 0.1 * g
            v = 0.95 * v_ref[piece, cut] + 0.05 * g * g
            m_ref[piece, cut] = m
            v_ref[piece, cut] = v
            mine[cut] = (w - 0.02 * (m * lax.rsqrt(v + 1e-8) + 0.1 * w)).astype(jnp.bfloat16)
            if c:
                gather(c - 1, 0, piece).start()
            else:

                @pl.when(piece > 0)
                def _():
                    gather(last, 0, piece - 1).start()

    for k in range(2 * hops):

        @pl.loop(0, pieces)
        def _(piece, k=k):
            for c in range(COLOURS):
                gather(c, k, piece).wait_recv()
                if k + 1 < 2 * hops:
                    gather(c, k + 1, piece).start()
                if k:
                    gather(c, k - 1, piece).wait_send()
            if k == 0:

                @pl.when(piece == 0)
                def _():
                    gather(last, 0, pieces - 1).start()

    @pl.loop(0, pieces)
    def _(piece):
        for c in range(COLOURS):
            gather(c, 2 * hops - 1, piece).wait_send()

    @pl.loop(1, n)
    def _(i):
        tell(i).wait_send()


def out_kernel(layers, state, whole, *refs):
    outs, sems = refs[:9], refs[9]
    copies = [
        pltpu.make_async_copy(source.at[piece], outs[3 * i + piece // layers].at[piece % layers], sems.at[i, piece])
        for i, source in enumerate((whole, state.at[0], state.at[1]))
        for piece in range(3 * layers)
    ]
    for copy in copies:
        copy.start()
    for copy in copies:
        copy.wait()


def solution(mesh):
    n = mesh.shape["dp"]
    side = math.isqrt(n)

    def step(*arrays):
        terms, weights, m, v = (arrays[i : i + 3] for i in (0, 3, 6, 9))
        layers = weights[0].shape[0]
        pieces = 3 * layers
        terms = [tiled(t[0], (layers, side, side)) for t in terms]
        whole = [tiled(w, (layers, side, side)) for w in weights]
        ms = [tiled(one, (layers,)) for one in m]
        vs = [tiled(one, (layers,)) for one in v]
        tiles = ms[0].shape[1]
        part = tiles // COLOURS
        assert side * side == n and tiles % COLOURS == 0 and all(one.shape[1] == tiles for one in ms)
        hops = side - 1
        any_space = pl.BlockSpec(memory_space=pl.ANY)
        vmem = pl.BlockSpec(memory_space=pltpu.VMEM)
        bf16, f32, dma = jnp.bfloat16, jnp.float32, pltpu.SemaphoreType.DMA
        count = float(sum(w.size for w in weights))
        new = pl.pallas_call(
            functools.partial(step_kernel, side, layers, count),
            out_shape=(
                pltpu.VMEM((2, pieces, tiles, 8, 128), f32),
                pltpu.VMEM((pieces, side, side, tiles, 8, 128), bf16),
            ),
            in_specs=[any_space] * 12,
            out_specs=(vmem,) * 2,
            scratch_shapes=[
                pltpu.VMEM((hops, COLOURS, pieces, side, part, 8, 128), bf16),
                pltpu.VMEM((hops, COLOURS, pieces, part, 8, 128), bf16),
                pltpu.VMEM((pieces, tiles, 8, 128), bf16),
                pltpu.VMEM((n, 8, 128), f32),
                pltpu.VMEM((8, 128), f32),
                dma((pieces,)),
                dma((3, pieces)),
                dma((2 * hops, COLOURS, pieces)),
                dma((2 * hops, COLOURS, pieces)),
                dma((n,)),
                dma((n,)),
            ],
            compiler_params=pltpu.CompilerParams(collective_id=0, has_side_effects=True, vmem_limit_bytes=27 * 2**20),
            name="step",
        )(*terms, *whole, *ms, *vs)
        new = [pltpu.with_memory_space_constraint(one, pltpu.VMEM) for one in new]
        shapes = [(layers, side, side, tiles, 8, 128)] * 3 + [(layers, tiles, 8, 128)] * 6
        outs = pl.pallas_call(
            functools.partial(out_kernel, layers),
            out_shape=[jax.ShapeDtypeStruct(s, bf16 if i < 3 else f32) for i, s in enumerate(shapes)],
            in_specs=[vmem] * 2,
            out_specs=[any_space] * 9,
            scratch_shapes=[dma((3, pieces))],
            compiler_params=pltpu.CompilerParams(vmem_limit_bytes=2**20),
            name="out",
        )(*new)
        return tuple(untiled(one, like.shape) for one, like in zip(outs, (*weights, *m, *v), strict=True))

    all_of, cut = P(None, None, None), P(None, "dp", None)
    return jax.shard_map(
        step,
        mesh=mesh,
        in_specs=(P(("rep", "dp"), None, None, None),) * 3 + (all_of,) * 3 + (cut,) * 6,
        out_specs=(P("rep", None, None),) * 3 + (P("rep", "dp", None),) * 6,
        check_vma=False,
    )
```

```python
import functools
import math

import jax
import jax.numpy as jnp
from jax import lax
from jax.experimental import pallas as pl
from jax.experimental.pallas import tpu as pltpu
from jax.sharding import PartitionSpec as P

MESH = pl.DeviceIdType.MESH
LATE_NS = 13_000
COLOURS = 4


def tiled(a, lead):
    rows, columns = a.shape[-2:]
    t = a.reshape(*a.shape[:-2], rows // 8, 8, columns // 128, 128)
    return jnp.swapaxes(t, -3, -2).reshape(*lead, -1, 8, 128)


def untiled(t, shape):
    rows, columns = shape[-2:]
    t = t.reshape(*shape[:-2], rows // 8, columns // 128, 8, 128)
    return jnp.swapaxes(t, -3, -2).reshape(shape)


def step_kernel(side, layers, count, *refs):
    n = side * side
    terms, weights, m_in, v_in = (refs[i : i + 3] for i in (0, 3, 6, 9))
    state, whole, first, second, own_w, squares, total, load, load3, send, recv, sq_send, sq_recv = refs[12:]
    m_ref, v_ref = state.at[0], state.at[1]
    pieces = whole.shape[0]
    tiles = whole.shape[3]
    part = tiles // COLOURS
    hops = side - 1
    me = lax.axis_index("dp")
    x, y = me // side, me % side

    def load_terms(piece):
        return pltpu.make_async_copy(terms[piece // layers].at[piece % layers], whole.at[piece], load.at[0])

    def load_state(piece):
        a, l = piece // layers, piece % layers
        return (
            pltpu.make_async_copy(weights[a].at[l, x, y], own_w.at[piece], load3.at[0]),
            pltpu.make_async_copy(m_in[a].at[l], m_ref.at[piece], load3.at[1]),
            pltpu.make_async_copy(v_in[a].at[l], v_ref.at[piece], load3.at[1]),
        )

    for piece in range(pieces):
        load_terms(piece).start()

    barrier = pltpu.get_barrier_semaphore()

    def place(c):
        way = 1 if c % 2 == 0 else -1
        return (x, y, way) if c < 2 else (y, x, way)

    def device(c, p, q):
        return p * side + q if c < 2 else q * side + p

    for c in range(COLOURS):
        p, q, way = place(c)
        pl.semaphore_signal(barrier, inc=1, device_id={"dp": device(c, (p + way + side) % side, q)}, device_id_type=MESH)
    pl.semaphore_wait(barrier, COLOURS)

    def row(c, piece, p):
        cut = pl.ds(c * part, part)
        return whole.at[piece, p, :, cut] if c < 2 else whole.at[piece, :, p, cut]

    def block(c, piece, p, q):
        cut = pl.ds(c * part, part)
        return whole.at[piece, p, q, cut] if c < 2 else whole.at[piece, q, p, cut]

    def wrap(i):
        return (i + 2 * side) % side

    def scatter(c, k, piece, own=None):
        p, q, way = place(c)
        if k < hops:
            source, target = row(c, piece, wrap(p - way * (k + 1))), first.at[k, c, piece]
            to = device(c, wrap(p + way), q)
            if own is not None:
                cut = pl.ds(c * part, part)
                own, i = own.at[piece % layers], wrap(p - way)
                source = own.at[i, :, cut] if c < 2 else own.at[:, i, cut]
        else:
            source, target = block(c, piece, p, wrap(q - way * (k - hops + 1))), second.at[k - hops, c, piece]
            to = device(c, p, wrap(q + way))
        return pltpu.make_async_remote_copy(
            src_ref=source, dst_ref=target, send_sem=send.at[k], recv_sem=recv.at[k, piece], device_id={"dp": to}, device_id_type=MESH
        )

    def landed(sem, *those):
        for one in those:
            pltpu.make_async_copy(one, one, sem).wait()

    def add(c, k, piece):
        p, q, way = place(c)
        if k < hops:
            mine, came = row(c, piece, wrap(p - way * (k + 2))), first.at[k, c, piece]

            @pl.loop(0, side)
            def _(i):
                mine[i] = (mine[i].astype(jnp.float32) + came[i].astype(jnp.float32)).astype(jnp.bfloat16)

        else:
            mine, came = block(c, piece, p, wrap(q - way * (k - hops + 2))), second.at[k - hops, c, piece]
            new = (mine[...].astype(jnp.float32) + came[...].astype(jnp.float32)).astype(jnp.bfloat16)
            mine[...] = new
            if k == 2 * hops - 1:
                g = new.astype(jnp.float32)
                total[...] += jnp.sum(g * g, axis=0)

    total[...] = jnp.zeros_like(total)

    @pl.when(lax.axis_index("rep") % 2 == 0)
    def _():
        pl.delay(LATE_NS)

    for piece in range(pieces):
        for c in range(COLOURS):
            scatter(c, 0, piece, terms[piece // layers]).start()
    for piece in range(pieces):
        for copy in load_state(piece):
            copy.start()

    last = COLOURS - 1
    landed(load.at[0], whole)
    for k in range(2 * hops):

        @pl.loop(0, pieces)
        def _(piece, k=k):
            landed(recv.at[k, piece], first.at[k, :, piece] if k < hops else second.at[k - hops, :, piece])
            for c in range(COLOURS):
                add(c, k, piece)
                if c:
                    if k + 1 < 2 * hops:
                        scatter(c - 1, k + 1, piece).start()
                    continue

                if k + 1 < 2 * hops:

                    @pl.when(piece > 0)
                    def _():
                        scatter(last, k + 1, piece - 1).start()

                if k:

                    @pl.when(piece == 0)
                    def _():
                        scatter(last, k, pieces - 1).start()

    for k in range(2 * hops - 1):
        landed(send.at[k], first.at[k] if k < hops else second.at[k - hops])

    def tell(i):
        return pltpu.make_async_remote_copy(
            src_ref=total, dst_ref=squares.at[i], send_sem=sq_send.at[0], recv_sem=sq_recv.at[0], device_id={"dp": (me + i) % n}, device_id_type=MESH
        )

    @pl.loop(1, n)
    def _(i):
        tell(i).start()

    squares[0] = total[...]

    landed(send.at[2 * hops - 1], second.at[hops - 1])
    landed(load3.at[0], own_w)
    landed(load3.at[1], state)
    landed(sq_recv.at[0], squares.at[pl.ds(1, n - 1)])

    of_all = jnp.sum(jnp.sum(squares[...], axis=0), keepdims=True)
    factor = jnp.minimum(1.0, 0.5 * lax.rsqrt(of_all / count + 1e-30))[None]

    def gather(c, k, piece):
        p, q, way = place(c)
        if k < hops:
            moved, to = block(c, piece, p, wrap(q - way * k)), device(c, p, wrap(q + way))
        else:
            moved, to = row(c, piece, wrap(p - way * (k - hops))), device(c, wrap(p + way), q)
        return pltpu.make_async_remote_copy(
            src_ref=moved, dst_ref=moved, send_sem=send.at[k], recv_sem=recv.at[k, piece], device_id={"dp": to}, device_id_type=MESH
        )

    @pl.loop(0, pieces)
    def _(piece):
        mine = whole.at[piece, x, y]
        for c in range(COLOURS):
            cut = pl.ds(c * part, part)
            g = mine[cut].astype(jnp.float32) * factor
            w = own_w[piece, cut].astype(jnp.float32)
            m = 0.9 * m_ref[piece, cut] + 0.1 * g
            v = 0.95 * v_ref[piece, cut] + 0.05 * g * g
            m_ref[piece, cut] = m
            v_ref[piece, cut] = v
            mine[cut] = (w - 0.02 * (m * lax.rsqrt(v + 1e-8) + 0.1 * w)).astype(jnp.bfloat16)
            if c:
                gather(c - 1, 0, piece).start()
            else:

                @pl.when(piece > 0)
                def _():
                    gather(last, 0, piece - 1).start()

    early = pieces - layers
    for k in range(2 * hops):

        @pl.loop(0, pieces if k < hops else early)
        def _(piece, k=k):
            landed(recv.at[k, piece], second.at[k, :, piece] if k < hops else first.at[k - hops, :, piece])

            @pl.when(piece < (pieces if k + 1 < hops else early if k + 1 < 2 * hops else 0))
            def _():
                for c in range(COLOURS):
                    gather(c, k + 1, piece).start()

            if k == 0:

                @pl.when(piece == 0)
                def _():
                    gather(last, 0, pieces - 1).start()

    for k in range(hops):
        landed(send.at[k], second.at[k])
        landed(send.at[k + hops], first.at[k, :, pl.ds(0, early)])
    landed(sq_send.at[0], squares.at[pl.ds(1, n - 1)])


def last_kernel(side, layers, whole, after, out, local, send, recv):
    pieces, tiles, hops = whole.shape[0], whole.shape[3], side - 1
    part = tiles // COLOURS
    me = lax.axis_index("dp")
    x, y = me // side, me % side

    def row(c, ref, piece, p):
        cut = pl.ds(c * part, part)
        return ref.at[piece, p, :, cut] if c < 2 else ref.at[piece, :, p, cut]

    def ahead(c, i):
        p, q = (x, y) if c < 2 else (y, x)
        p = (p + i * (1 if c % 2 == 0 else -1) + 2 * side) % side
        return p, {"dp": p * side + q if c < 2 else q * side + p}

    def own(c, piece):
        p = ahead(c, 0)[0]
        return row(c, whole, pieces - layers + piece, p), row(c, out, piece, p)

    def gather(c, k, piece):
        moved = row(c, out, piece, ahead(c, -k)[0])
        return pltpu.make_async_remote_copy(
            src_ref=own(c, piece)[0] if k == 0 else moved, dst_ref=moved, send_sem=send.at[k], recv_sem=recv.at[k, piece], device_id=ahead(c, 1)[1], device_id_type=MESH
        )

    barrier = pltpu.get_barrier_semaphore()
    for c in range(COLOURS):
        pl.semaphore_signal(barrier, inc=1, device_id=ahead(c, 1)[1], device_id_type=MESH)
    pl.semaphore_wait(barrier, COLOURS)

    for piece in range(layers):
        for c in range(COLOURS):
            gather(c, 0, piece).start()
    for piece in range(layers):
        for c in range(COLOURS):
            pltpu.make_async_copy(*own(c, piece), local.at[0]).start()
    for k in range(hops):
        for piece in range(layers):
            pltpu.make_async_copy(out.at[0, 0], out.at[0, 0], recv.at[k, piece]).wait()
            if k + 1 < hops:
                for c in range(COLOURS):
                    gather(c, k + 1, piece).start()
    for k in range(hops):
        pltpu.make_async_copy(out.at[:, 0], out.at[:, 0], send.at[k]).wait()
    pltpu.make_async_copy(out.at[:, 0], out.at[:, 0], local.at[0]).wait()


def out_kernel(layers, state, whole, *refs):
    outs, done, sems = refs[:8], refs[8], refs[9]
    early = whole.shape[0] - layers
    done[...] = jnp.zeros_like(done)
    copies = [pltpu.make_async_copy(whole.at[i], outs[i // layers].at[i % layers], sems.at[0]) for i in range(early)]
    copies += [
        pltpu.make_async_copy(state.at[j, i], outs[2 + 3 * j + i // layers].at[i % layers], sems.at[1])
        for j in range(2)
        for i in range(3 * layers)
    ]
    for copy in copies:
        copy.start()
    for i, all_of_it in enumerate((whole.at[pl.ds(0, early)], state)):
        pltpu.make_async_copy(all_of_it, all_of_it, sems.at[i]).wait()


def last_out_kernel(last, out, sem):
    copy = pltpu.make_async_copy(last, out, sem)
    copy.start()
    copy.wait()


def solution(mesh):
    n = mesh.shape["dp"]
    side = math.isqrt(n)

    def step(*arrays):
        terms, weights, m, v = (arrays[i : i + 3] for i in (0, 3, 6, 9))
        layers = weights[0].shape[0]
        pieces = 3 * layers
        terms = [tiled(t[0], (layers, side, side)) for t in terms]
        whole = [tiled(w, (layers, side, side)) for w in weights]
        ms = [tiled(one, (layers,)) for one in m]
        vs = [tiled(one, (layers,)) for one in v]
        tiles = ms[0].shape[1]
        part = tiles // COLOURS
        assert side * side == n and tiles % COLOURS == 0 and all(one.shape[1] == tiles for one in ms)
        hops = side - 1
        any_space = pl.BlockSpec(memory_space=pl.ANY)
        vmem = pl.BlockSpec(memory_space=pltpu.VMEM)
        bf16, f32, dma = jnp.bfloat16, jnp.float32, pltpu.SemaphoreType.DMA
        count = float(sum(w.size for w in weights))
        new = pl.pallas_call(
            functools.partial(step_kernel, side, layers, count),
            out_shape=(
                pltpu.VMEM((2, pieces, tiles, 8, 128), f32),
                pltpu.VMEM((pieces, side, side, tiles, 8, 128), bf16),
            ),
            in_specs=[any_space] * 12,
            out_specs=(vmem,) * 2,
            scratch_shapes=[
                pltpu.VMEM((hops, COLOURS, pieces, side, part, 8, 128), bf16),
                pltpu.VMEM((hops, COLOURS, pieces, part, 8, 128), bf16),
                pltpu.VMEM((pieces, tiles, 8, 128), bf16),
                pltpu.VMEM((n, 8, 128), f32),
                pltpu.VMEM((8, 128), f32),
                dma((1,)),
                dma((2,)),
                dma((2 * hops,)),
                dma((2 * hops, pieces)),
                dma((1,)),
                dma((1,)),
            ],
            compiler_params=pltpu.CompilerParams(collective_id=0, has_side_effects=True, vmem_limit_bytes=27 * 2**20),
            name="step",
        )(*terms, *whole, *ms, *vs)
        state, gathered = (pltpu.with_memory_space_constraint(one, pltpu.VMEM) for one in new)
        one, block = (layers, side, side, tiles, 8, 128), (layers, tiles, 8, 128)
        *outs, after = pl.pallas_call(
            functools.partial(out_kernel, layers),
            out_shape=[jax.ShapeDtypeStruct(one, bf16)] * 2 + [jax.ShapeDtypeStruct(block, f32)] * 6 + [jax.ShapeDtypeStruct((8, 128), f32)],
            in_specs=[vmem] * 2,
            out_specs=[any_space] * 8 + [vmem],
            scratch_shapes=[dma((2,))],
            compiler_params=pltpu.CompilerParams(vmem_limit_bytes=2**20),
            name="out",
        )(state, gathered)
        last = pl.pallas_call(
            functools.partial(last_kernel, side, layers),
            out_shape=pltpu.VMEM(one, bf16),
            in_specs=[vmem, any_space],
            out_specs=vmem,
            scratch_shapes=[dma((1,)), dma((hops,)), dma((hops, layers))],
            compiler_params=pltpu.CompilerParams(collective_id=1, has_side_effects=True, vmem_limit_bytes=2**20),
            name="last",
        )(gathered, after)
        last = pl.pallas_call(
            last_out_kernel,
            out_shape=jax.ShapeDtypeStruct(one, bf16),
            in_specs=[vmem],
            out_specs=any_space,
            scratch_shapes=[dma],
            compiler_params=pltpu.CompilerParams(vmem_limit_bytes=2**20),
            name="last_out",
        )(pltpu.with_memory_space_constraint(last, pltpu.VMEM))
        outs = [*outs[:2], last, *outs[2:]]
        return tuple(untiled(one, like.shape) for one, like in zip(outs, (*weights, *m, *v), strict=True))

    all_of, cut = P(None, None, None), P(None, "dp", None)
    return jax.shard_map(
        step,
        mesh=mesh,
        in_specs=(P(("rep", "dp"), None, None, None),) * 3 + (all_of,) * 3 + (cut,) * 6,
        out_specs=(P("rep", None, None),) * 3 + (P("rep", "dp", None),) * 6,
        check_vma=False,
    )
```

```python
import functools
import math

import jax
import jax.numpy as jnp
from jax import lax
from jax.experimental import pallas as pl
from jax.experimental.pallas import tpu as pltpu
from jax.sharding import PartitionSpec as P

MESH = pl.DeviceIdType.MESH
LATE_NS = 13_000
COLOURS = 4


def tiled(a, lead):
    rows, columns = a.shape[-2:]
    t = a.reshape(*a.shape[:-2], rows // 8, 8, columns // 128, 128)
    return jnp.swapaxes(t, -3, -2).reshape(*lead, -1, 8, 128)


def untiled(t, shape):
    rows, columns = shape[-2:]
    t = t.reshape(*shape[:-2], rows // 8, columns // 128, 8, 128)
    return jnp.swapaxes(t, -3, -2).reshape(shape)


def step_kernel(side, layers, count, *refs):
    n = side * side
    terms, weights, m_in, v_in = (refs[i : i + 3] for i in (0, 3, 6, 9))
    state, whole, first, second, own_w, squares, total, load, load3, send, recv, sq_send, sq_recv = refs[12:]
    m_ref, v_ref = state.at[0], state.at[1]
    pieces = whole.shape[0]
    tiles = whole.shape[3]
    part = tiles // COLOURS
    hops = side - 1
    me = lax.axis_index("dp")
    x, y = me // side, me % side

    def load_terms(piece):
        return pltpu.make_async_copy(terms[piece // layers].at[piece % layers], whole.at[piece], load.at[0])

    def load_state(piece):
        a, l = piece // layers, piece % layers
        return (
            pltpu.make_async_copy(weights[a].at[l, x, y], own_w.at[piece], load3.at[0]),
            pltpu.make_async_copy(m_in[a].at[l], m_ref.at[piece], load3.at[1]),
            pltpu.make_async_copy(v_in[a].at[l], v_ref.at[piece], load3.at[1]),
        )

    for piece in range(pieces):
        load_terms(piece).start()

    barrier = pltpu.get_barrier_semaphore()

    def place(c):
        way = 1 if c % 2 == 0 else -1
        return (x, y, way) if c < 2 else (y, x, way)

    def device(c, p, q):
        return p * side + q if c < 2 else q * side + p

    for c in range(COLOURS):
        p, q, way = place(c)
        pl.semaphore_signal(barrier, inc=1, device_id={"dp": device(c, (p + way + side) % side, q)}, device_id_type=MESH)
    pl.semaphore_wait(barrier, COLOURS)

    def row(c, piece, p):
        cut = pl.ds(c * part, part)
        return whole.at[piece, p, :, cut] if c < 2 else whole.at[piece, :, p, cut]

    def block(c, piece, p, q):
        cut = pl.ds(c * part, part)
        return whole.at[piece, p, q, cut] if c < 2 else whole.at[piece, q, p, cut]

    def wrap(i):
        return (i + 2 * side) % side

    def scatter(c, k, piece, own=None):
        p, q, way = place(c)
        if k < hops:
            source, target = row(c, piece, wrap(p - way * (k + 1))), first.at[k, c, piece]
            to = device(c, wrap(p + way), q)
            if own is not None:
                cut = pl.ds(c * part, part)
                own, i = own.at[piece % layers], wrap(p - way)
                source = own.at[i, :, cut] if c < 2 else own.at[:, i, cut]
        else:
            source, target = block(c, piece, p, wrap(q - way * (k - hops + 1))), second.at[k - hops, c, piece]
            to = device(c, p, wrap(q + way))
        return pltpu.make_async_remote_copy(
            src_ref=source, dst_ref=target, send_sem=send.at[k], recv_sem=recv.at[k, piece], device_id={"dp": to}, device_id_type=MESH
        )

    def landed(sem, *those):
        for one in those:
            pltpu.make_async_copy(one, one, sem).wait()

    def add(c, k, piece):
        p, q, way = place(c)
        if k < hops:
            mine, came = row(c, piece, wrap(p - way * (k + 2))), first.at[k, c, piece]

            @pl.loop(0, side)
            def _(i):
                mine[i] = (mine[i].astype(jnp.float32) + came[i].astype(jnp.float32)).astype(jnp.bfloat16)

        else:
            mine, came = block(c, piece, p, wrap(q - way * (k - hops + 2))), second.at[k - hops, c, piece]
            new = (mine[...].astype(jnp.float32) + came[...].astype(jnp.float32)).astype(jnp.bfloat16)
            mine[...] = new
            if k == 2 * hops - 1:
                g = new.astype(jnp.float32)
                total[...] += jnp.sum(g * g, axis=0)

    total[...] = jnp.zeros_like(total)

    @pl.when(lax.axis_index("rep") % 2 == 0)
    def _():
        pl.delay(LATE_NS)

    for piece in range(pieces):
        for c in range(COLOURS):
            scatter(c, 0, piece, terms[piece // layers]).start()
    for piece in range(pieces):
        for copy in load_state(piece):
            copy.start()

    last = COLOURS - 1
    landed(load.at[0], whole)
    for k in range(2 * hops):

        @pl.loop(0, pieces)
        def _(piece, k=k):
            landed(recv.at[k, piece], first.at[k, :, piece] if k < hops else second.at[k - hops, :, piece])
            for c in range(COLOURS):
                add(c, k, piece)
                if c:
                    if k + 1 < 2 * hops:
                        scatter(c - 1, k + 1, piece).start()
                    continue

                if k + 1 < 2 * hops:

                    @pl.when(piece > 0)
                    def _():
                        scatter(last, k + 1, piece - 1).start()

                if k:

                    @pl.when(piece == 0)
                    def _():
                        scatter(last, k, pieces - 1).start()

    for k in range(2 * hops - 1):
        landed(send.at[k], first.at[k] if k < hops else second.at[k - hops])

    def tell(i):
        return pltpu.make_async_remote_copy(
            src_ref=total, dst_ref=squares.at[i], send_sem=sq_send.at[0], recv_sem=sq_recv.at[0], device_id={"dp": (me + i) % n}, device_id_type=MESH
        )

    @pl.loop(1, n)
    def _(i):
        tell(i).start()

    squares[0] = total[...]

    landed(send.at[2 * hops - 1], second.at[hops - 1])
    landed(load3.at[0], own_w)
    landed(load3.at[1], state)
    landed(sq_recv.at[0], squares.at[pl.ds(1, n - 1)])

    of_all = jnp.sum(jnp.sum(squares[...], axis=0), keepdims=True)
    factor = jnp.minimum(1.0, 0.5 * lax.rsqrt(of_all / count + 1e-30))[None]

    def gather(c, k, piece):
        p, q, way = place(c)
        if k < hops:
            moved, to = block(c, piece, p, wrap(q - way * k)), device(c, p, wrap(q + way))
        else:
            moved, to = row(c, piece, wrap(p - way * (k - hops))), device(c, wrap(p + way), q)
        return pltpu.make_async_remote_copy(
            src_ref=moved, dst_ref=moved, send_sem=send.at[k], recv_sem=recv.at[k, piece], device_id={"dp": to}, device_id_type=MESH
        )

    @pl.loop(0, pieces)
    def _(piece):
        mine = whole.at[piece, x, y]
        for c in range(COLOURS):
            cut = pl.ds(c * part, part)
            g = mine[cut].astype(jnp.float32) * factor
            w = own_w[piece, cut].astype(jnp.float32)
            m = 0.9 * m_ref[piece, cut] + 0.1 * g
            v = 0.95 * v_ref[piece, cut] + 0.05 * g * g
            m_ref[piece, cut] = m
            v_ref[piece, cut] = v
            mine[cut] = (w - 0.02 * (m * lax.rsqrt(v + 1e-8) + 0.1 * w)).astype(jnp.bfloat16)
            if c:
                gather(c - 1, 0, piece).start()
            else:

                @pl.when(piece > 0)
                def _():
                    gather(last, 0, piece - 1).start()

    early = pieces - layers
    for k in range(2 * hops):

        @pl.loop(0, pieces if k < hops else early)
        def _(piece, k=k):
            landed(recv.at[k, piece], second.at[k, :, piece] if k < hops else first.at[k - hops, :, piece])

            @pl.when(piece < (pieces if k + 1 < hops else early if k + 1 < 2 * hops else 0))
            def _():
                for c in range(COLOURS):
                    gather(c, k + 1, piece).start()

            if k == 0:

                @pl.when(piece == 0)
                def _():
                    gather(last, 0, pieces - 1).start()

    for k in range(hops):
        landed(send.at[k], second.at[k])
        landed(send.at[k + hops], first.at[k, :, pl.ds(0, early)])
    landed(sq_send.at[0], squares.at[pl.ds(1, n - 1)])


def last_kernel(side, layers, whole, after, out, send, recv):
    pieces, tiles, hops = whole.shape[0], whole.shape[3], side - 1
    part = tiles // COLOURS
    me = lax.axis_index("dp")
    x, y = me // side, me % side

    def row(c, ref, piece, p):
        cut = pl.ds(c * part, part)
        return ref.at[piece, p, :, cut] if c < 2 else ref.at[piece, :, p, cut]

    def ahead(c, i):
        p, q = (x, y) if c < 2 else (y, x)
        p = (p + i * (1 if c % 2 == 0 else -1) + 2 * side) % side
        return p, {"dp": p * side + q if c < 2 else q * side + p}

    def own(c, piece):
        p = ahead(c, 0)[0]
        return row(c, whole, pieces - layers + piece, p), row(c, out, piece, p)

    def gather(c, k, piece):
        moved = row(c, out, piece, ahead(c, -k)[0])
        return pltpu.make_async_remote_copy(
            src_ref=own(c, piece)[0] if k == 0 else moved, dst_ref=moved, send_sem=send.at[k], recv_sem=recv.at[k, piece], device_id=ahead(c, 1)[1], device_id_type=MESH
        )

    barrier = pltpu.get_barrier_semaphore()
    for c in range(COLOURS):
        pl.semaphore_signal(barrier, inc=1, device_id=ahead(c, 1)[1], device_id_type=MESH)
    pl.semaphore_wait(barrier, COLOURS)

    for piece in range(layers):
        for c in range(COLOURS):
            gather(c, 0, piece).start()
    for k in range(hops):
        for piece in range(layers):
            pltpu.make_async_copy(out.at[0, 0], out.at[0, 0], recv.at[k, piece]).wait()
            if k + 1 < hops:
                for c in range(COLOURS):
                    gather(c, k + 1, piece).start()
    for k in range(hops):
        pltpu.make_async_copy(out.at[:, 0], out.at[:, 0], send.at[k]).wait()


def row_of(side, c, ref, piece, i):
    part = ref.shape[3] // COLOURS
    me = lax.axis_index("dp")
    p = ((me // side if c < 2 else me % side) + i * (1 if c % 2 == 0 else -1) + 2 * side) % side
    cut = pl.ds(c * part, part)
    return ref.at[piece, p, :, cut] if c < 2 else ref.at[piece, :, p, cut]


def out_kernel(side, layers, state, whole, *refs):
    outs, done, sems = refs[:9], refs[9], refs[10]
    early = whole.shape[0] - layers
    done[...] = jnp.zeros_like(done)
    copies = [pltpu.make_async_copy(whole.at[i], outs[i // layers].at[i % layers], sems.at[0]) for i in range(early)]
    copies += [
        pltpu.make_async_copy(row_of(side, c, whole, early + i, 0), row_of(side, c, outs[2], i, 0), sems.at[2])
        for i in range(layers)
        for c in range(COLOURS)
    ]
    copies += [
        pltpu.make_async_copy(state.at[j, i], outs[3 + 3 * j + i // layers].at[i % layers], sems.at[1])
        for j in range(2)
        for i in range(3 * layers)
    ]
    for copy in copies:
        copy.start()
    for i, all_of_it in enumerate((whole.at[pl.ds(0, early)], state, whole.at[pl.ds(0, layers), 0])):
        pltpu.make_async_copy(all_of_it, all_of_it, sems.at[i]).wait()


def last_out_kernel(side, last, so_far, out, sem):
    layers = last.shape[0]
    for piece in range(layers):
        for c in range(COLOURS):
            for i in range(1, side):
                pltpu.make_async_copy(row_of(side, c, last, piece, i), row_of(side, c, out, piece, i), sem).start()
    others = last.at[:, pl.ds(1, side - 1)]
    pltpu.make_async_copy(others, others, sem).wait()


def solution(mesh):
    n = mesh.shape["dp"]
    side = math.isqrt(n)

    def step(*arrays):
        terms, weights, m, v = (arrays[i : i + 3] for i in (0, 3, 6, 9))
        layers = weights[0].shape[0]
        pieces = 3 * layers
        terms = [tiled(t[0], (layers, side, side)) for t in terms]
        whole = [tiled(w, (layers, side, side)) for w in weights]
        ms = [tiled(one, (layers,)) for one in m]
        vs = [tiled(one, (layers,)) for one in v]
        tiles = ms[0].shape[1]
        part = tiles // COLOURS
        assert side * side == n and tiles % COLOURS == 0 and all(one.shape[1] == tiles for one in ms)
        hops = side - 1
        any_space = pl.BlockSpec(memory_space=pl.ANY)
        vmem = pl.BlockSpec(memory_space=pltpu.VMEM)
        bf16, f32, dma = jnp.bfloat16, jnp.float32, pltpu.SemaphoreType.DMA
        count = float(sum(w.size for w in weights))
        new = pl.pallas_call(
            functools.partial(step_kernel, side, layers, count),
            out_shape=(
                pltpu.VMEM((2, pieces, tiles, 8, 128), f32),
                pltpu.VMEM((pieces, side, side, tiles, 8, 128), bf16),
            ),
            in_specs=[any_space] * 12,
            out_specs=(vmem,) * 2,
            scratch_shapes=[
                pltpu.VMEM((hops, COLOURS, pieces, side, part, 8, 128), bf16),
                pltpu.VMEM((hops, COLOURS, pieces, part, 8, 128), bf16),
                pltpu.VMEM((pieces, tiles, 8, 128), bf16),
                pltpu.VMEM((n, 8, 128), f32),
                pltpu.VMEM((8, 128), f32),
                dma((1,)),
                dma((2,)),
                dma((2 * hops,)),
                dma((2 * hops, pieces)),
                dma((1,)),
                dma((1,)),
            ],
            compiler_params=pltpu.CompilerParams(collective_id=0, has_side_effects=True, vmem_limit_bytes=27 * 2**20),
            name="step",
        )(*terms, *whole, *ms, *vs)
        state, gathered = (pltpu.with_memory_space_constraint(one, pltpu.VMEM) for one in new)
        one, block = (layers, side, side, tiles, 8, 128), (layers, tiles, 8, 128)
        *outs, after = pl.pallas_call(
            functools.partial(out_kernel, side, layers),
            out_shape=[jax.ShapeDtypeStruct(one, bf16)] * 3 + [jax.ShapeDtypeStruct(block, f32)] * 6 + [jax.ShapeDtypeStruct((8, 128), f32)],
            in_specs=[vmem] * 2,
            out_specs=[any_space] * 9 + [vmem],
            scratch_shapes=[dma((3,))],
            compiler_params=pltpu.CompilerParams(vmem_limit_bytes=2**20),
            name="out",
        )(state, gathered)
        last = pl.pallas_call(
            functools.partial(last_kernel, side, layers),
            out_shape=pltpu.VMEM(one, bf16),
            in_specs=[vmem, any_space],
            out_specs=vmem,
            scratch_shapes=[dma((hops,)), dma((hops, layers))],
            compiler_params=pltpu.CompilerParams(collective_id=1, has_side_effects=True, vmem_limit_bytes=2**20),
            name="last",
        )(gathered, after)
        outs[2] = pl.pallas_call(
            functools.partial(last_out_kernel, side),
            out_shape=jax.ShapeDtypeStruct(one, bf16),
            in_specs=[vmem, any_space],
            out_specs=any_space,
            input_output_aliases={1: 0},
            scratch_shapes=[dma],
            compiler_params=pltpu.CompilerParams(vmem_limit_bytes=2**20),
            name="last_out",
        )(pltpu.with_memory_space_constraint(last, pltpu.VMEM), outs[2])
        return tuple(untiled(one, like.shape) for one, like in zip(outs, (*weights, *m, *v), strict=True))

    all_of, cut = P(None, None, None), P(None, "dp", None)
    return jax.shard_map(
        step,
        mesh=mesh,
        in_specs=(P(("rep", "dp"), None, None, None),) * 3 + (all_of,) * 3 + (cut,) * 6,
        out_specs=(P("rep", None, None),) * 3 + (P("rep", "dp", None),) * 6,
        check_vma=False,
    )
```
